128 devices in a mesh: dp: 1, vp: 128 (over z, y, x, core).
Axes of the slice: x: 4, y: 4, z: 4, core: 2. Of those that a mesh axis runs over, the one named last changes fastest.
Arguments:
- hidden: bfloat16 [256, 32, 640], P('vp', 'dp')
- norm_gain: float32 [640], replicated
- norm_bias: float32 [640], replicated
- w_out: bfloat16 [640, 262144], P(None, 'vp')
- labels: int32 [256, 32], P('vp', 'dp')
- loss_mask: float32 [256, 32], P('vp', 'dp')
Outputs:
- output 1: float32 [1], P('dp')
- output 2: bfloat16 [256, 32, 640], P('vp', 'dp')
- output 3: float32 [640, 262144], P('dp', 'vp')
- output 4: float32 [640], P('dp')
- output 5: float32 [640], P('dp')
All inputs are finite; a program needn't handle non-finite values.
Results may differ from the reference program's by a relative error of at most 0.001.
Values are sent between devices in bfloat16 or wider.
A program may use at most 1 GiB of HBM per device.

```python
import jax
import jax.numpy as jnp
from jax import lax

SEQ_DEV = 2
GROUP_SIZE = 128
BATCH_PART = 32
D_MODEL = 640
VOCAB_SIZE = 262144
VOCAB_PAD = 262144
NORM_EPS = 1e-5
SEQ_LEN = SEQ_DEV * GROUP_SIZE
BLOCK_TOKENS = SEQ_DEV * BATCH_PART


def draw_labels(rng_key):
    key_pick, key_flat, key_upper, key_inner, key_skew = jax.random.split(rng_key, 5)
    tok_shape = (SEQ_LEN, BATCH_PART)
    flat_ids = jax.random.randint(key_flat, tok_shape, 0, VOCAB_SIZE)
    upper_one = jax.random.randint(key_upper, tok_shape, 1, VOCAB_SIZE + 1)
    upper_two = jax.random.randint(key_inner, tok_shape, 1, upper_one + 1)
    skew_ids = jax.random.randint(key_skew, tok_shape, 0, upper_two)
    pick_flat = jax.random.randint(key_pick, tok_shape, 0, 2)
    label_ids = jnp.where(pick_flat == 0, flat_ids, skew_ids)
    label_ids = label_ids.at[0, 0].set(VOCAB_SIZE - 1)
    return label_ids.at[SEQ_LEN - 1, BATCH_PART - 1].set(0)


def draw_mask(rng_key):
    mask_ids = jax.random.randint(rng_key, (SEQ_LEN, BATCH_PART), 0, 4)
    return (mask_ids > 0).astype(jnp.float32).at[0, 0].set(1.0)


def setup_inputs(seed: int = 0, part: int = 0) -> dict:
    root_key = jax.random.key(seed)
    shared_key, part_base = jax.random.split(root_key)
    part_key = jax.random.fold_in(part_base, part)
    key_w, key_g, key_c = jax.random.split(shared_key, 3)
    key_x, key_lab, key_mask = jax.random.split(part_key, 3)
    hidden = jax.random.normal(key_x, (SEQ_LEN, BATCH_PART, D_MODEL), jnp.float32).astype(jnp.bfloat16)
    norm_gain = 0.3 * jax.random.normal(key_g, (D_MODEL,), jnp.float32)
    norm_bias = 0.5 * jax.random.normal(key_c, (D_MODEL,), jnp.float32)
    w_out = (jax.random.normal(key_w, (D_MODEL, VOCAB_PAD), jnp.float32) * (2.0 / D_MODEL ** 0.5)).astype(jnp.bfloat16)
    labels = draw_labels(key_lab)
    loss_mask = draw_mask(key_mask)
    return {"hidden": hidden, "norm_gain": norm_gain, "norm_bias": norm_bias, "w_out": w_out, "labels": labels, "loss_mask": loss_mask}


def reference(hidden, norm_gain, norm_bias, w_out, labels, loss_mask):
    mask_total = jnp.sum(loss_mask)
    x_blocks = hidden.reshape(GROUP_SIZE, BLOCK_TOKENS, D_MODEL)
    lab_blocks = labels.reshape(GROUP_SIZE, BLOCK_TOKENS)
    mask_blocks = loss_mask.reshape(GROUP_SIZE, BLOCK_TOKENS)
    col_ids = jnp.arange(VOCAB_PAD, dtype=jnp.int32)

    def block_step(acc_state, block_in):
        grad_w, loss_sum, gain_sum, bias_sum = acc_state
        x_blk, lab_blk, mask_blk = block_in
        x_float = x_blk.astype(jnp.float32)
        tok_mean = jnp.mean(x_float, axis=-1, keepdims=True)
        centered = x_float - tok_mean
        inv_std = lax.rsqrt(jnp.mean(centered * centered, axis=-1, keepdims=True) + NORM_EPS)
        normed = centered * inv_std
        h_blk = (normed * (1.0 + norm_gain) + norm_bias).astype(jnp.bfloat16)
        logits = jnp.dot(h_blk, w_out, preferred_element_type=jnp.float32)
        row_max = jnp.max(logits, axis=-1, keepdims=True)
        exp_shift = jnp.exp(logits - row_max)
        sum_exp = jnp.sum(exp_shift, axis=-1, keepdims=True)
        is_label = (col_ids[None, :] == lab_blk[:, None]).astype(jnp.float32)
        target = jnp.sum(logits * is_label, axis=-1)
        tok_loss = row_max[:, 0] + jnp.log(sum_exp[:, 0]) - target
        tok_weight = mask_blk / mask_total
        grad_logits = ((exp_shift / sum_exp - is_label) * tok_weight[:, None]).astype(jnp.bfloat16)
        grad_w = grad_w + jnp.dot(h_blk.T, grad_logits, preferred_element_type=jnp.float32)
        grad_h = jnp.dot(grad_logits, w_out.T, preferred_element_type=jnp.float32)
        gain_sum = gain_sum + jnp.sum(grad_h * normed, axis=0)
        bias_sum = bias_sum + jnp.sum(grad_h, axis=0)
        scaled = grad_h * (1.0 + norm_gain)
        grad_x = inv_std * (scaled - jnp.mean(scaled, axis=-1, keepdims=True) - normed * jnp.mean(scaled * normed, axis=-1, keepdims=True))
        loss_sum = loss_sum + jnp.sum(mask_blk * tok_loss)
        return (grad_w, loss_sum, gain_sum, bias_sum), grad_x.astype(jnp.bfloat16)

    init_state = (jnp.zeros((D_MODEL, VOCAB_PAD), jnp.float32), jnp.zeros((), jnp.float32), jnp.zeros((D_MODEL,), jnp.float32), jnp.zeros((D_MODEL,), jnp.float32))
    final_state, grad_x = lax.scan(block_step, init_state, (x_blocks, lab_blocks, mask_blocks))
    grad_w, loss_sum, gain_sum, bias_sum = final_state
    loss = (loss_sum / mask_total).reshape(1)
    return loss, grad_x.reshape(SEQ_LEN, BATCH_PART, D_MODEL), grad_w, gain_sum, bias_sum
```

```python
import jax
import jax.numpy as jnp
from jax import lax
from jax.experimental import pallas as pl
from jax.experimental.pallas import tpu as pltpu
from jax.sharding import PartitionSpec as P

NORM_EPS = 1e-5
F32 = jnp.float32
BF16 = jnp.bfloat16
SIDE = 4
ORDERS = (("x", "y", "z"), ("y", "z", "x"), ("z", "x", "y"))
AXPOS = {"z": 0, "y": 1, "x": 2}
TOK = 64
DM = 640
VL = 2048
NTOK = 4096
TB = 512
NB = NTOK // TB
CT = 1024
VMEM_CAP = 64 * 1024 * 1024 - 65536


def here():
    me = lax.axis_index("vp")
    chip = me // 2
    return {"core": me % 2, "x": chip % SIDE, "y": (chip // SIDE) % SIDE, "z": chip // (SIDE * SIDE)}


def dev_of(pos):
    return ((pos["z"] * SIDE + pos["y"]) * SIDE + pos["x"]) * 2 + pos["core"]


def shifted(pos, axis, delta):
    out = dict(pos)
    if axis == "core":
        out["core"] = 1 - pos["core"]
    else:
        out[axis] = (pos[axis] + delta + SIDE) % SIDE
    return {"vp": dev_of(out)}


def barrier_with(peers):
    sem = pltpu.get_barrier_semaphore()
    for peer in peers:
        pl.semaphore_signal(sem, inc=1, device_id=peer, device_id_type=pl.DeviceIdType.MESH)
    pl.semaphore_wait(sem, len(peers))


def ring_peers(pos, deltas):
    return [shifted(pos, ax, d) for ax in ("x", "y", "z") for d in deltas] + [shifted(pos, "core", 0)]


def rcopy(src, dst, ssem, rsem, peer):
    return pltpu.make_async_remote_copy(src_ref=src, dst_ref=dst, send_sem=ssem, recv_sem=rsem,
                                        device_id=peer, device_id_type=pl.DeviceIdType.MESH)


def gather_kernel(h0, h1, h2, w_in, g0, g1, g2, w_oth, ssem, rsem, lsem, wsem):
    pos = here()
    barrier_with(ring_peers(pos, (1, -1)))
    wcopy = rcopy(w_in, w_oth, wsem.at[0], wsem.at[1], shifted(pos, "core", 0))
    wcopy.start()
    hs, gs = (h0, h1, h2), (g0, g1, g2)
    local = []
    for c in range(3):
        cp = pltpu.make_async_copy(hs[c], gs[c].at[pos["z"], pos["y"], pos["x"]], lsem.at[c])
        cp.start()
        local.append(cp)

    def unit(c, phase, coord):
        axis = ORDERS[c][phase]
        done = ORDERS[c][:phase]
        idx = []
        for ax in ("z", "y", "x"):
            if ax in done:
                idx.append(slice(None))
            elif ax == axis:
                idx.append(coord)
            else:
                idx.append(pos[ax])
        return tuple(idx)

    sends = []
    for phase in range(3):
        first = {}
        for c in range(3):
            axis = ORDERS[c][phase]
            me = pos[axis]
            if phase == 1:
                local[c].wait()
            for k, d in ((0, 1), (1, -1)):
                slot = (c * 3 + phase) * 4 + k
                own = gs[c].at[unit(c, phase, me)]
                src = hs[c] if phase == 0 else own
                cp = rcopy(src, own, ssem.at[slot], rsem.at[slot], shifted(pos, axis, d))
                cp.start()
                sends.append(cp)
                first[c, k] = cp
        second = []
        for c in range(3):
            axis = ORDERS[c][phase]
            me = pos[axis]
            for k, d in ((0, 1), (1, -1)):
                slot = (c * 3 + phase) * 4 + 2 + k
                first[c, k].wait_recv()
                blk = gs[c].at[unit(c, phase, (me - d + SIDE) % SIDE)]
                half = blk.at[(slice(None),) * (phase + 1) + (pl.ds(128 * k, 128),)]
                cp = rcopy(half, half, ssem.at[slot], rsem.at[slot], shifted(pos, axis, d))
                cp.start()
                sends.append(cp)
                second.append(cp)
        for cp in second:
            cp.wait_recv()
    for cp in sends:
        cp.wait_send()
    wcopy.wait()


def gather_call(h0, h1, h2, w_blk):
    vm = pl.BlockSpec(memory_space=pltpu.VMEM)
    anyspec = pl.BlockSpec(memory_space=pl.ANY)
    gshape = jax.ShapeDtypeStruct((SIDE, SIDE, SIDE, TOK, 256), BF16)
    return pl.pallas_call(
        gather_kernel,
        out_shape=(gshape, gshape, gshape, jax.ShapeDtypeStruct((DM, VL), BF16)),
        in_specs=[vm, vm, vm, anyspec],
        out_specs=(vm, vm, vm, anyspec),
        scratch_shapes=[pltpu.SemaphoreType.DMA((36,)), pltpu.SemaphoreType.DMA((36,)),
                        pltpu.SemaphoreType.DMA((3,)), pltpu.SemaphoreType.DMA((2,))],
        compiler_params=pltpu.CompilerParams(collective_id=1, has_side_effects=True, vmem_limit_bytes=VMEM_CAP),
    )(h0, h1, h2, w_blk)


def label_minus_lane(aux):
    lab = aux[:, 0:1] + aux[:, 1:2] * 256.0 + aux[:, 2:3] * 65536.0
    lane = lax.broadcasted_iota(jnp.int32, (aux.shape[0], 128), 1)
    return lab.astype(jnp.int32) - lane


def logits_kernel(g0, g1, g2, w_own, w_oth, z_own, z_oth, lse_out, mt_out, ms_out,
                  zA, zB, m_s, s_s, t_s, lab_s, sem):
    pos = here()
    base_own = dev_of(pos) * VL
    base_oth = dev_of({**pos, "core": 1 - pos["core"]}) * VL
    zbuf = (zA, zB)
    tiles = ((w_own, z_own, 0, base_own), (w_own, z_own, CT, base_own), (w_oth, z_oth, 0, base_oth), (w_oth, z_oth, CT, base_oth))
    mt_out[...] = jnp.zeros_like(mt_out)
    ms_out[...] = jnp.zeros_like(ms_out)

    def stats(buf, cbase, first, rows):
        zt = buf[rows, :]
        tile_max = zt[:, 0:128]
        for k in range(1, CT // 128):
            tile_max = jnp.maximum(tile_max, zt[:, 128 * k:128 * k + 128])
        labm = lab_s[rows, :]
        if first:
            m_new = tile_max
        else:
            m_old = m_s[rows, :]
            m_new = jnp.maximum(m_old, tile_max)
        acc = None
        tacc = None
        for k in range(CT // 128):
            zk = zt[:, 128 * k:128 * k + 128]
            e = jnp.exp(zk - m_new)
            hit = jnp.where(labm == cbase + 128 * k, zk, 0.0)
            acc = e if acc is None else acc + e
            tacc = hit if tacc is None else tacc + hit
        if first:
            s_s[rows, :] = acc
            t_s[rows, :] = tacc
        else:
            s_s[rows, :] = s_s[rows, :] * jnp.exp(m_old - m_new) + acc
            t_s[rows, :] = t_s[rows, :] + tacc
        m_s[rows, :] = m_new

    def block(i, carry):
        tok = pl.ds(pl.multiple_of(i * TB, TB), TB)
        a0 = g0[tok, :]
        a1 = g1[tok, :]
        a2 = g2[tok, 0:128]
        aux = g2[tok, 128:256].astype(F32)
        lab_s[...] = label_minus_lane(aux)
        for seg in range(5):
            if seg < 4:
                w_ref, z_ref, off, _ = tiles[seg]
                buf = zbuf[seg % 2]
                out = pltpu.make_async_copy(buf, z_ref.at[tok, pl.ds(off, CT)], sem.at[seg % 2])
                if seg >= 2:
                    out.wait()
                else:
                    @pl.when(i > 0)
                    def _():
                        out.wait()
            for sub in range(4):
                if seg < 4:
                    cols = pl.ds(off + 256 * sub, 256)
                    zt = jnp.dot(a0, w_ref[0:256, cols], preferred_element_type=F32)
                    zt += jnp.dot(a1, w_ref[256:512, cols], preferred_element_type=F32)
                    zt += jnp.dot(a2, w_ref[512:640, cols], preferred_element_type=F32)
                    buf[:, 256 * sub:256 * sub + 256] = zt
                if seg > 0:
                    _, _, poff, pbase = tiles[seg - 1]
                    for r in range(8):
                        stats(zbuf[(seg - 1) % 2], pbase + poff, seg == 1, pl.ds(sub * 128 + r * 16, 16))
            if seg < 4:
                out.start()
        mt = m_s[...].T
        st = s_s[...].T
        mx = jnp.max(mt, axis=0, keepdims=True)
        tot = jnp.sum(st * jnp.exp(mt - mx), axis=0, keepdims=True)
        lse_out[pl.ds(i, 1), :] = mx + jnp.log(tot)
        mcol = aux[:, 3:4]
        mt_out[...] += jnp.sum((t_s[...] * mcol).reshape(TB // 8, 8, 128), axis=0)
        ms_out[...] += jnp.sum(jnp.broadcast_to(mcol, (TB, 128)).reshape(TB // 8, 8, 128), axis=0)
        return carry

    lax.fori_loop(0, NB, block, 0)
    for k in range(2):
        pltpu.make_async_copy(zbuf[k], z_oth.at[pl.ds(0, TB), pl.ds(0, CT)], sem.at[k]).wait()


def logits_call(g0, g1, g2, w_own, w_oth):
    vm = pl.BlockSpec(memory_space=pltpu.VMEM)
    anyspec = pl.BlockSpec(memory_space=pl.ANY)
    zshape = jax.ShapeDtypeStruct((NTOK, VL), F32)
    return pl.pallas_call(
        logits_kernel,
        out_shape=(zshape, zshape, jax.ShapeDtypeStruct((NB, TB), F32), jax.ShapeDtypeStruct((8, 128), F32), jax.ShapeDtypeStruct((8, 128), F32)),
        in_specs=[vm] * 5,
        out_specs=(anyspec, anyspec, vm, vm, vm),
        scratch_shapes=[pltpu.VMEM((TB, CT), F32), pltpu.VMEM((TB, CT), F32)] + [pltpu.VMEM((TB, 128), F32)] * 3
        + [pltpu.VMEM((TB, 128), jnp.int32), pltpu.SemaphoreType.DMA((2,))],
        compiler_params=pltpu.CompilerParams(vmem_limit_bytes=VMEM_CAP),
    )(g0, g1, g2, w_own, w_oth)


def lse_kernel(lse_in, ms_in, lse_out, ms_out, cur, got, mgot, ssem, rsem):
    pos = here()
    barrier_with(ring_peers(pos, (1, 2, 3)))
    mcopy = rcopy(ms_in, mgot, ssem.at[9], rsem.at[9], shifted(pos, "core", 0))
    mcopy.start()
    for p, axis in enumerate(("x", "y", "z")):
        src = lse_in if p == 0 else cur.at[p - 1]
        cps = []
        for d in (2, 1, 3):
            k = p * 3 + d - 1
            cp = rcopy(src, got.at[k], ssem.at[k], rsem.at[k], shifted(pos, axis, d))
            cp.start()
            cps.append(cp)
        for cp in cps:
            cp.wait()
        v = [src[...], got[p * 3], got[p * 3 + 1], got[p * 3 + 2]]
        mx = jnp.maximum(jnp.maximum(v[0], v[1]), jnp.maximum(v[2], v[3]))
        tot = (jnp.exp(v[0] - mx) + jnp.exp(v[1] - mx)) + (jnp.exp(v[2] - mx) + jnp.exp(v[3] - mx))
        res = mx + jnp.log(tot)
        if p < 2:
            cur[p] = res
        else:
            lse_out[...] = res
    mcopy.wait()
    tot = jnp.sum(ms_in[...] + mgot[...], axis=0, keepdims=True)
    ms_out[...] = jnp.broadcast_to(tot, ms_out.shape)


def lse_call(lse_loc, msum):
    vm = pl.BlockSpec(memory_space=pltpu.VMEM)
    return pl.pallas_call(
        lse_kernel,
        out_shape=(jax.ShapeDtypeStruct((NB, TB), F32), jax.ShapeDtypeStruct((8, 128), F32)),
        in_specs=[vm, vm],
        out_specs=(vm, vm),
        scratch_shapes=[pltpu.VMEM((2, NB, TB), F32), pltpu.VMEM((9, NB, TB), F32), pltpu.VMEM((8, 128), F32),
                        pltpu.SemaphoreType.DMA((10,)), pltpu.SemaphoreType.DMA((10,))],
        compiler_params=pltpu.CompilerParams(collective_id=2, has_side_effects=True),
    )(lse_loc, msum)


def grads_kernel(g0, g1, g2, w_own, w_oth, z_own, z_oth, lse, msum, dh_out, dw_own, dw_oth,
                 zA, zB, dA, dB, hT, dh_s, lse_s, wt_s, lab_s, zsem, osem):
    pos = here()
    base_own = dev_of(pos) * VL
    base_oth = dev_of({**pos, "core": 1 - pos["core"]}) * VL
    zbuf, dbuf = (zA, zB), (dA, dB)
    tiles = ((w_own, z_own, 0, base_own, dw_own), (w_own, z_own, CT, base_own, dw_own),
             (w_oth, z_oth, 0, base_oth, dw_oth), (w_oth, z_oth, CT, base_oth, dw_oth))

    def zcopy(i, t):
        _, z_ref, off, _, _ = tiles[t]
        tok = pl.ds(pl.multiple_of(i * TB, TB), TB)
        return pltpu.make_async_copy(z_ref.at[tok, pl.ds(off, CT)], zbuf[t % 2], zsem.at[t % 2])

    def prep(i):
        tok = pl.ds(pl.multiple_of(i * TB, TB), TB)
        aux = g2[tok, 128:256].astype(F32)
        lab_s[...] = label_minus_lane(aux)
        wt_s[...] = jnp.broadcast_to(aux[:, 3:4], (TB, 128)) / msum[0:1, :]
        lse_s[...] = jnp.broadcast_to(lse[pl.ds(i, 1), :], (128, TB)).T

    def make_dz(t, r):
        _, _, off, base, _ = tiles[t]
        rows = pl.ds(r * 16, 16)
        lse_b = lse_s[rows, :]
        wt = wt_s[rows, :]
        labm = lab_s[rows, :]
        for k in range(CT // 128):
            ks = slice(128 * k, 128 * k + 128)
            p = jnp.exp(zbuf[t % 2][rows, ks] - lse_b)
            p = jnp.where(labm == base + off + 128 * k, p - 1.0, p)
            dbuf[t % 2][rows, ks] = (p * wt).astype(BF16)

    dw_own[...] = jnp.zeros_like(dw_own)
    dw_oth[...] = jnp.zeros_like(dw_oth)
    zcopy(0, 0).start()
    zcopy(0, 1).start()
    prep(0)
    zcopy(0, 0).wait()
    for r in range(TB // 16):
        make_dz(0, r)
    zcopy(0, 2).start()

    def block(i, carry):
        tok = pl.ds(pl.multiple_of(i * TB, TB), TB)
        hT[0:256, :] = g0[tok, :].T
        hT[256:512, :] = g1[tok, :].T
        hT[512:640, :] = g2[tok, 0:128].T
        for seg in range(4):
            w_ref, _, off, _, dw_ref = tiles[seg]
            dz = dbuf[seg % 2]
            nt = (seg + 1) % 4
            if seg == 3:
                nxt = jnp.minimum(i + 1, NB - 1)
                prep(nxt)
            else:
                nxt = i
            zcopy(nxt, nt).wait()
            piece = 0
            for n in range(3):
                lo, hi = 256 * n, min(256 * n + 256, DM)
                part = lax.dot_general(dz[...], w_ref[lo:hi, pl.ds(off, CT)], (((1,), (1,)), ((), ())), preferred_element_type=F32)
                if seg == 0:
                    dh_s[:, lo:hi] = part
                else:
                    dh_s[:, lo:hi] += part
                for r in range(4):
                    make_dz(nt, piece)
                    piece += 1
            for sub in range(4):
                cols = pl.ds(off + 256 * sub, 256)
                dw_ref[:, cols] += jnp.dot(hT[...], dz[:, 256 * sub:256 * sub + 256], preferred_element_type=F32)
                for r in range(5):
                    make_dz(nt, piece)
                    piece += 1
            after = jnp.minimum(i + (seg + 3) // 4, NB - 1)
            zcopy(after, (seg + 3) % 4).start()
        return carry

    def block_out(i, carry):
        block(i, carry)
        tok = pl.ds(pl.multiple_of(i * TB, TB), TB)
        cp = pltpu.make_async_copy(dh_s, dh_out.at[tok, :], osem.at[0])
        cp.start()
        cp.wait()
        return carry

    lax.fori_loop(0, NB, block_out, 0)
    zcopy(NB - 1, 1).wait()
    zcopy(NB - 1, 2).wait()


def grads_call(g0, g1, g2, w_own, w_oth, z_own, z_oth, lse, msum):
    vm = pl.BlockSpec(memory_space=pltpu.VMEM)
    anyspec = pl.BlockSpec(memory_space=pl.ANY)
    dwshape = jax.ShapeDtypeStruct((DM, VL), F32)
    return pl.pallas_call(
        grads_kernel,
        out_shape=(jax.ShapeDtypeStruct((NTOK, DM), F32), dwshape, dwshape),
        in_specs=[vm] * 5 + [anyspec] * 2 + [vm] * 2,
        out_specs=(anyspec, vm, vm),
        scratch_shapes=[pltpu.VMEM((TB, CT), F32)] * 2 + [pltpu.VMEM((TB, CT), BF16)] * 2
        + [pltpu.VMEM((DM, TB), BF16), pltpu.VMEM((TB, DM), F32)] + [pltpu.VMEM((TB, 128), F32)] * 2
        + [pltpu.VMEM((TB, 128), jnp.int32), pltpu.SemaphoreType.DMA((2,)), pltpu.SemaphoreType.DMA((1,))],
        compiler_params=pltpu.CompilerParams(vmem_limit_bytes=VMEM_CAP),
    )(g0, g1, g2, w_own, w_oth, z_own, z_oth, lse, msum)


LANES = ((0, 256), (256, 256), (512, 128))


def scatter_kernel(dh, normed, inv_std, gain, lossp, dw_send, dx_out, vec_out, dw_got, *scr):
    bufs = scr[:36]
    vcur, vgot, own_s, ssem, rsem, vssem, vrsem, wsem = scr[36:]
    pos = here()
    barrier_with(ring_peers(pos, (1, 2, 3)))
    wcopy = rcopy(dw_send, dw_got, wsem.at[0], wsem.at[1], shifted(pos, "core", 0))
    wcopy.start()
    half = TOK // 2
    waits = []
    cur = {}

    def view(c, phase, coord, lo):
        lane0, width = LANES[c]
        axis = ORDERS[c][phase]
        rows = pl.ds(lo, half)
        if phase == 0:
            idx = tuple(coord if ax == axis else slice(None) for ax in ("z", "y", "x"))
            return dh.at[idx + (rows, pl.ds(lane0, width))]
        ref, axes = cur[c]
        idx = tuple(coord if ax == axis else slice(None) for ax in axes)
        return ref.at[idx + (rows, slice(None))]

    def add_into(dst, srcs, lead):
        if lead == 0:
            v = dst[...]
            for s in srcs:
                v = v + s[...]
            dst[...] = v
        else:
            def body(j, carry):
                if lead == 1:
                    add_into(dst.at[j], [s.at[j] for s in srcs], 0)
                else:
                    for q in range(SIDE):
                        add_into(dst.at[j, q], [s.at[j, q] for s in srcs], 0)
                return carry
            lax.fori_loop(0, SIDE, body, 0)

    for phase in range(3):
        lead = 2 - phase
        state = []
        for c in range(3):
            axis = ORDERS[c][phase]
            a = pos[axis]
            r1p, r1m, r2p, r2m = bufs[(c * 3 + phase) * 4:(c * 3 + phase) * 4 + 4]
            s0 = (c * 3 + phase) * 6
            pre = (slice(None),) * lead
            right, left = shifted(pos, axis, 1), shifted(pos, axis, -1)
            lo0, lo1 = pre + (pl.ds(0, half), slice(None)), pre + (pl.ds(half, half), slice(None))
            near_r, near_l = (a + 1) % SIDE, (a + SIDE - 1) % SIDE
            far = (a + 2) % SIDE
            sends = [
                rcopy(view(c, phase, far, 0), r1p, ssem.at[s0], rsem.at[s0], right),
                rcopy(view(c, phase, far, half), r1m, ssem.at[s0 + 1], rsem.at[s0 + 1], left),
                rcopy(view(c, phase, near_r, half), r2p.at[lo1], ssem.at[s0 + 2], rsem.at[s0 + 2], right),
                rcopy(view(c, phase, near_l, 0), r2m.at[lo0], ssem.at[s0 + 3], rsem.at[s0 + 3], left),
                rcopy(r1p, r2p.at[lo0], ssem.at[s0 + 4], rsem.at[s0 + 4], right),
                rcopy(r1m, r2m.at[lo1], ssem.at[s0 + 5], rsem.at[s0 + 5], left),
            ]
            for cp in sends[:4]:
                cp.start()
            state.append((sends, r1p, r1m, r2p, r2m, near_r, near_l, a))
        for c in range(3):
            sends, r1p, r1m, r2p, r2m, near_r, near_l, a = state[c]
            sends[0].wait_recv()
            add_into(r1p, [view(c, phase, near_r, 0)], lead)
            sends[4].start()
            sends[1].wait_recv()
            add_into(r1m, [view(c, phase, near_l, half)], lead)
            sends[5].start()
        new = {}
        for c in range(3):
            sends, r1p, r1m, r2p, r2m, near_r, near_l, a = state[c]
            for k in range(2, 6):
                sends[k].wait_recv()
            for lo in (0, half):
                sl = (slice(None),) * lead + (pl.ds(lo, half), slice(None))
                add_into(r2p.at[sl], [r2m.at[sl], view(c, phase, a, lo)], lead)
            axes = tuple(ax for ax in ("z", "y", "x") if ax not in ORDERS[c][:phase + 1])
            new[c] = (r2p, axes)
            waits += sends
        cur.update(new)
    gh = jnp.concatenate([cur[c][0][...] for c in range(3)], axis=1)
    nrm = normed[...]
    dg = jnp.sum(gh * nrm, axis=0, keepdims=True)
    dc = jnp.sum(gh, axis=0, keepdims=True)
    lane_loss = lossp[...]
    for k in range(5):
        own_s[k:k + 1, :] = dg[:, 128 * k:128 * k + 128]
        own_s[5 + k:6 + k, :] = dc[:, 128 * k:128 * k + 128]
    own_s[10:16, :] = jnp.zeros((6, 128), F32)
    own_s[10:11, :] = jnp.sum(lane_loss, axis=0, keepdims=True)
    src = own_s
    slot = 0
    for p, axis in enumerate(("core", "x", "y", "z")):
        deltas = (1,) if axis == "core" else (2, 1, 3)
        cps = []
        for d in deltas:
            cp = rcopy(src, vgot.at[slot], vssem.at[slot], vrsem.at[slot], shifted(pos, axis, d))
            cp.start()
            cps.append((cp, slot))
            slot += 1
        if p == 0:
            q = gh * (1.0 + gain[...])
            cen = q - jnp.mean(q, axis=-1, keepdims=True)
            dx_out[...] = (inv_std[...] * (cen - nrm * jnp.mean(q * nrm, axis=-1, keepdims=True))).astype(BF16)
        for cp, _ in cps:
            cp.wait()
        vals = {d: vgot[s] for d, (_, s) in zip(deltas, cps)}
        if axis == "core":
            tot = src[...] + vals[1]
        else:
            tot = (src[...] + vals[2]) + (vals[1] + vals[3])
        if p < 3:
            vcur[p] = tot
            src = vcur.at[p]
        else:
            vec_out[...] = tot
    for cp in waits:
        cp.wait_send()
    wcopy.wait()


def scatter_call(dh, normed, inv_std, gain, lossp, dw_oth):
    vm = pl.BlockSpec(memory_space=pltpu.VMEM)
    anyspec = pl.BlockSpec(memory_space=pl.ANY)
    half = TOK // 2
    bufs = []
    for c in range(3):
        for phase in range(3):
            lead = (SIDE,) * (2 - phase)
            w = LANES[c][1]
            bufs += [pltpu.VMEM(lead + (half, w), F32)] * 2 + [pltpu.VMEM(lead + (TOK, w), F32)] * 2
    return pl.pallas_call(
        scatter_kernel,
        out_shape=(jax.ShapeDtypeStruct((TOK, DM), BF16), jax.ShapeDtypeStruct((16, 128), F32), jax.ShapeDtypeStruct((DM, VL), F32)),
        in_specs=[vm] * 5 + [anyspec],
        out_specs=(vm, vm, anyspec),
        scratch_shapes=bufs + [pltpu.VMEM((3, 16, 128), F32), pltpu.VMEM((10, 16, 128), F32), pltpu.VMEM((16, 128), F32),
                               pltpu.SemaphoreType.DMA((54,)), pltpu.SemaphoreType.DMA((54,)),
                               pltpu.SemaphoreType.DMA((10,)), pltpu.SemaphoreType.DMA((10,)), pltpu.SemaphoreType.DMA((2,))],
        compiler_params=pltpu.CompilerParams(collective_id=3, has_side_effects=True, vmem_limit_bytes=VMEM_CAP),
    )(dh, normed, inv_std, gain, lossp, dw_oth)


def solution(mesh):
    def per_device(hidden, norm_gain, norm_bias, w_blk, labels, loss_mask):
        x = hidden.reshape(TOK, DM).astype(F32)
        centered = x - jnp.mean(x, axis=-1, keepdims=True)
        inv_std = lax.rsqrt(jnp.mean(centered * centered, axis=-1, keepdims=True) + NORM_EPS)
        normed = centered * inv_std
        h = (normed * (1.0 + norm_gain) + norm_bias).astype(BF16)
        lab = labels.reshape(TOK, 1)
        mask = loss_mask.reshape(TOK, 1)
        lane = lax.broadcasted_iota(jnp.int32, (TOK, 128), 1)
        aux = jnp.where(lane == 0, lab % 256, jnp.where(lane == 1, (lab // 256) % 256, jnp.where(lane == 2, lab // 65536, 0))).astype(F32)
        aux = jnp.where(lane == 3, mask, aux).astype(BF16)
        h2 = jnp.concatenate([h[:, 512:], aux], axis=1)
        g0, g1, g2, w_oth = gather_call(h[:, :256], h[:, 256:512], h2, w_blk)
        g0, g1, g2 = (g.reshape(NTOK, 256) for g in (g0, g1, g2))
        z_own, z_oth, lse_loc, mt, ms = logits_call(g0, g1, g2, w_blk, w_oth)
        lse, msum = lse_call(lse_loc, ms)
        dh, dw_own, dw_oth = grads_call(g0, g1, g2, w_blk, w_oth, z_own, z_oth, lse, msum)
        chip = lax.axis_index("vp") // 2
        own_lse = lax.dynamic_slice(lse.reshape(NTOK), (chip * TOK,), (TOK,))
        loss_lane = jnp.concatenate([mask[:, 0] * own_lse, jnp.zeros((64,), F32)]).reshape(1, 128)
        lossp = jnp.concatenate([-mt, loss_lane, jnp.zeros((7, 128), F32)])
        dx, vec, dw_got = scatter_call(dh.reshape(SIDE, SIDE, SIDE, TOK, DM), normed, jnp.broadcast_to(inv_std, (TOK, DM)),
                                       norm_gain.reshape(1, DM), lossp, dw_oth)
        grad_w = dw_own + dw_got
        loss = jnp.sum(vec[10]) / msum[0, 0]
        return (loss.reshape(1), dx.reshape(hidden.shape), grad_w, vec[0:5].reshape(DM), vec[5:10].reshape(DM))

    tok_spec = P("vp", "dp")
    return jax.shard_map(
        per_device,
        mesh=mesh,
        in_specs=(P("vp", "dp", None), P(None), P(None), P(None, "vp"), tok_spec, tok_spec),
        out_specs=(P("dp"), P("vp", "dp", None), P("dp", "vp"), P("dp"), P("dp")),
        check_vma=False,
    )
```

```python
import jax
import jax.numpy as jnp
from jax import lax
from jax.experimental import pallas as pl
from jax.experimental.pallas import tpu as pltpu
from jax.sharding import PartitionSpec as P

NORM_EPS = 1e-5
F32 = jnp.float32
BF16 = jnp.bfloat16
SIDE = 4
ORDERS = (("x", "y", "z"), ("y", "z", "x"), ("z", "x", "y"))
AXPOS = {"z": 0, "y": 1, "x": 2}
TOK = 64
DM = 640
VL = 2048
NTOK = 4096
TB = 512
NB = NTOK // TB
CT = 1024
NSEG = 2 * VL // CT
VMEM_CAP = 64 * 1024 * 1024 - 65536


def here():
    me = lax.axis_index("vp")
    chip = me // 2
    return {"core": me % 2, "x": chip % SIDE, "y": (chip // SIDE) % SIDE, "z": chip // (SIDE * SIDE)}


def dev_of(pos):
    return ((pos["z"] * SIDE + pos["y"]) * SIDE + pos["x"]) * 2 + pos["core"]


def shifted(pos, axis, delta):
    out = dict(pos)
    if axis == "core":
        out["core"] = 1 - pos["core"]
    else:
        out[axis] = (pos[axis] + delta + SIDE) % SIDE
    return {"vp": dev_of(out)}


def barrier_with(peers):
    sem = pltpu.get_barrier_semaphore()
    for peer in peers:
        pl.semaphore_signal(sem, inc=1, device_id=peer, device_id_type=pl.DeviceIdType.MESH)
    pl.semaphore_wait(sem, len(peers))


def ring_peers(pos, deltas):
    return [shifted(pos, ax, d) for ax in ("x", "y", "z") for d in deltas] + [shifted(pos, "core", 0)]


def rcopy(src, dst, ssem, rsem, peer):
    return pltpu.make_async_remote_copy(src_ref=src, dst_ref=dst, send_sem=ssem, recv_sem=rsem,
                                        device_id=peer, device_id_type=pl.DeviceIdType.MESH)


def gather_kernel(h0, h1, h2, w_in, g0, g1, g2, w_oth, ssem, rsem, lsem, wsem):
    pos = here()
    barrier_with(ring_peers(pos, (1, -1)))
    wcopy = rcopy(w_in, w_oth, wsem.at[0], wsem.at[1], shifted(pos, "core", 0))
    wcopy.start()
    hs, gs = (h0, h1, h2), (g0, g1, g2)
    local = []
    for c in range(3):
        cp = pltpu.make_async_copy(hs[c], gs[c].at[pos["z"], pos["y"], pos["x"]], lsem.at[c])
        cp.start()
        local.append(cp)

    def unit(c, phase, coord):
        axis = ORDERS[c][phase]
        done = ORDERS[c][:phase]
        idx = []
        for ax in ("z", "y", "x"):
            if ax in done:
                idx.append(slice(None))
            elif ax == axis:
                idx.append(coord)
            else:
                idx.append(pos[ax])
        return tuple(idx)

    sends = []
    for phase in range(3):
        first = {}
        for c in range(3):
            axis = ORDERS[c][phase]
            me = pos[axis]
            if phase == 1:
                local[c].wait()
            for k, d in ((0, 1), (1, -1)):
                slot = (c * 3 + phase) * 4 + k
                own = gs[c].at[unit(c, phase, me)]
                src = hs[c] if phase == 0 else own
                cp = rcopy(src, own, ssem.at[slot], rsem.at[slot], shifted(pos, axis, d))
                cp.start()
                sends.append(cp)
                first[c, k] = cp
        second = []
        for c in range(3):
            axis = ORDERS[c][phase]
            me = pos[axis]
            for k, d in ((0, 1), (1, -1)):
                slot = (c * 3 + phase) * 4 + 2 + k
                first[c, k].wait_recv()
                blk = gs[c].at[unit(c, phase, (me - d + SIDE) % SIDE)]
                half = blk.at[(slice(None),) * phase + (k,)]
                cp = rcopy(half, half, ssem.at[slot], rsem.at[slot], shifted(pos, axis, d))
                cp.start()
                sends.append(cp)
                second.append(cp)
        for cp in second:
            cp.wait_recv()
    for cp in sends:
        cp.wait_send()
    wcopy.wait()


def gather_call(h0, h1, h2, w_blk):
    vm = pl.BlockSpec(memory_space=pltpu.VMEM)
    anyspec = pl.BlockSpec(memory_space=pl.ANY)
    gshape = jax.ShapeDtypeStruct((SIDE, SIDE, SIDE, 2, TOK, 128), BF16)
    return pl.pallas_call(
        gather_kernel,
        out_shape=(gshape, gshape, gshape, jax.ShapeDtypeStruct((DM, VL), BF16)),
        in_specs=[vm, vm, vm, anyspec],
        out_specs=(vm, vm, vm, anyspec),
        scratch_shapes=[pltpu.SemaphoreType.DMA((36,)), pltpu.SemaphoreType.DMA((36,)),
                        pltpu.SemaphoreType.DMA((3,)), pltpu.SemaphoreType.DMA((2,))],
        compiler_params=pltpu.CompilerParams(collective_id=1, has_side_effects=True, vmem_limit_bytes=VMEM_CAP),
    )(h0, h1, h2, w_blk)


def label_minus_lane(aux):
    lab = aux[:, 0:1] + aux[:, 1:2] * 256.0 + aux[:, 2:3] * 65536.0
    lane = lax.broadcasted_iota(jnp.int32, (aux.shape[0], 128), 1)
    return lab.astype(jnp.int32) - lane


def tok_tile(g_ref, i, k):
    return g_ref[pl.ds(i * (TB // TOK), TB // TOK), k].reshape(TB, 128)


def load_w(w_own, w_oth, wt, wsem):
    cps = []
    for half, ref in enumerate((w_own, w_oth)):
        for k in range(VL // 128):
            cp = pltpu.make_async_copy(ref.at[:, pl.ds(128 * k, 128)], wt.at[half * (VL // 128) + k], wsem.at[half * (VL // 128) + k])
            cp.start()
            cps.append(cp)
    for cp in cps:
        cp.wait()


def w_pair(wt, j, lo, hi):
    return jnp.concatenate([wt[2 * j, lo:hi, :], wt[2 * j + 1, lo:hi, :]], axis=1)


def logits_kernel(g0, g1, g2, w_own, w_oth, z_out, lse_out, mt_out, ms_out,
                  zb, wt, m_s, s_s, t_s, lab_s, sem, wsem):
    pos = here()
    base_own = dev_of(pos) * VL
    base_oth = dev_of({**pos, "core": 1 - pos["core"]}) * VL
    load_w(w_own, w_oth, wt, wsem)
    mt_out[...] = jnp.zeros_like(mt_out)
    ms_out[...] = jnp.zeros_like(ms_out)

    def stats(buf, seg, cbase, rows):
        c0 = seg * CT
        nk = CT // 128
        tile_max = buf[rows, pl.ds(c0, 128)]
        for k in range(1, nk):
            tile_max = jnp.maximum(tile_max, buf[rows, pl.ds(c0 + 128 * k, 128)])
        labm = lab_s[rows, :]
        if seg == 0:
            m_new = tile_max
        else:
            m_old = m_s[rows, :]
            m_new = jnp.maximum(m_old, tile_max)
        acc = None
        tacc = None
        for k in range(nk):
            zk = buf[rows, pl.ds(c0 + 128 * k, 128)]
            e = jnp.exp(zk - m_new)
            hit = jnp.where(labm == cbase + 128 * k, zk, 0.0)
            acc = e if acc is None else acc + e
            tacc = hit if tacc is None else tacc + hit
        if seg == 0:
            s_s[rows, :] = acc
            t_s[rows, :] = tacc
        else:
            s_s[rows, :] = s_s[rows, :] * jnp.exp(m_old - m_new) + acc
            t_s[rows, :] = t_s[rows, :] + tacc
        m_s[rows, :] = m_new

    def zcopy(i):
        return pltpu.make_async_copy(zb.at[i % 2], z_out.at[pl.ds(pl.multiple_of(i * TB, TB), TB), :], sem.at[i % 2])

    def block(i, carry):
        @pl.when(i >= 2)
        def _():
            zcopy(i - 2).wait()
        buf = zb.at[i % 2]
        a0 = jnp.concatenate([tok_tile(g0, i, 0), tok_tile(g0, i, 1)], axis=1)
        a1 = jnp.concatenate([tok_tile(g1, i, 0), tok_tile(g1, i, 1)], axis=1)
        a2 = tok_tile(g2, i, 0)
        aux = tok_tile(g2, i, 1).astype(F32)
        lab_s[...] = label_minus_lane(aux)
        nsub = CT // 256
        nrow = TB // 16 // nsub
        for seg in range(NSEG + 1):
            for sub in range(nsub):
                if seg < NSEG:
                    j = seg * nsub + sub
                    zt = jnp.dot(a0, w_pair(wt, j, 0, 256), preferred_element_type=F32)
                    zt += jnp.dot(a1, w_pair(wt, j, 256, 512), preferred_element_type=F32)
                    zt += jnp.dot(a2, w_pair(wt, j, 512, 640), preferred_element_type=F32)
                    buf[:, 256 * j:256 * j + 256] = zt
                if seg > 0:
                    half = (seg - 1) // (NSEG // 2)
                    cbase = (base_own, base_oth)[half] + ((seg - 1) % (NSEG // 2)) * CT
                    for r in range(nrow):
                        stats(buf, seg - 1, cbase, pl.ds((sub * nrow + r) * 16, 16))
        mt = m_s[...].T
        st = s_s[...].T
        mx = jnp.max(mt, axis=0, keepdims=True)
        tot = jnp.sum(st * jnp.exp(mt - mx), axis=0, keepdims=True)
        lse_out[pl.ds(i, 1), :] = mx + jnp.log(tot)
        mcol = aux[:, 3:4]
        mt_out[...] += jnp.sum((t_s[...] * mcol).reshape(TB // 8, 8, 128), axis=0)
        ms_out[...] += jnp.sum(jnp.broadcast_to(mcol, (TB, 128)).reshape(TB // 8, 8, 128), axis=0)
        zcopy(i).start()
        return carry

    lax.fori_loop(0, NB, block, 0)
    zcopy(NB - 2).wait()
    zcopy(NB - 1).wait()


def logits_call(g0, g1, g2, w_own, w_oth):
    vm = pl.BlockSpec(memory_space=pltpu.VMEM)
    anyspec = pl.BlockSpec(memory_space=pl.ANY)
    return pl.pallas_call(
        logits_kernel,
        out_shape=(jax.ShapeDtypeStruct((NTOK, 2 * VL), F32), jax.ShapeDtypeStruct((NB, TB), F32), jax.ShapeDtypeStruct((8, 128), F32), jax.ShapeDtypeStruct((8, 128), F32)),
        in_specs=[vm] * 3 + [anyspec] * 2,
        out_specs=(anyspec, vm, vm, vm),
        scratch_shapes=[pltpu.VMEM((2, TB, 2 * VL), F32), pltpu.VMEM((2 * VL // 128, DM, 128), BF16)] + [pltpu.VMEM((TB, 128), F32)] * 3
        + [pltpu.VMEM((TB, 128), jnp.int32), pltpu.SemaphoreType.DMA((2,)), pltpu.SemaphoreType.DMA((2 * VL // 128,))],
        compiler_params=pltpu.CompilerParams(vmem_limit_bytes=VMEM_CAP),
    )(g0, g1, g2, w_own, w_oth)


def lse_kernel(lse_in, ms_in, lse_out, ms_out, cur, got, mgot, ssem, rsem):
    pos = here()
    barrier_with(ring_peers(pos, (1, 2, 3)))
    mcopy = rcopy(ms_in, mgot, ssem.at[9], rsem.at[9], shifted(pos, "core", 0))
    mcopy.start()
    for p, axis in enumerate(("x", "y", "z")):
        src = lse_in if p == 0 else cur.at[p - 1]
        cps = []
        for d in (2, 1, 3):
            k = p * 3 + d - 1
            cp = rcopy(src, got.at[k], ssem.at[k], rsem.at[k], shifted(pos, axis, d))
            cp.start()
            cps.append(cp)
        for cp in cps:
            cp.wait()
        v = [src[...], got[p * 3], got[p * 3 + 1], got[p * 3 + 2]]
        mx = jnp.maximum(jnp.maximum(v[0], v[1]), jnp.maximum(v[2], v[3]))
        tot = (jnp.exp(v[0] - mx) + jnp.exp(v[1] - mx)) + (jnp.exp(v[2] - mx) + jnp.exp(v[3] - mx))
        res = mx + jnp.log(tot)
        if p < 2:
            cur[p] = res
        else:
            lse_out[...] = res
    mcopy.wait()
    tot = jnp.sum(ms_in[...] + mgot[...], axis=0, keepdims=True)
    ms_out[...] = jnp.broadcast_to(tot, ms_out.shape)


def lse_call(lse_loc, msum):
    vm = pl.BlockSpec(memory_space=pltpu.VMEM)
    return pl.pallas_call(
        lse_kernel,
        out_shape=(jax.ShapeDtypeStruct((NB, TB), F32), jax.ShapeDtypeStruct((8, 128), F32)),
        in_specs=[vm, vm],
        out_specs=(vm, vm),
        scratch_shapes=[pltpu.VMEM((2, NB, TB), F32), pltpu.VMEM((9, NB, TB), F32), pltpu.VMEM((8, 128), F32),
                        pltpu.SemaphoreType.DMA((10,)), pltpu.SemaphoreType.DMA((10,))],
        compiler_params=pltpu.CompilerParams(collective_id=2, has_side_effects=True),
    )(lse_loc, msum)


def grads_kernel(g0, g1, g2, w_own, w_oth, z_in, lse, msum, dh_out, dw_own, dw_oth,
                 zb, db, wt, hT, dh_s, lse_s, wt_s, lab_s, zsem, osem, wsem):
    pos = here()
    base_own = dev_of(pos) * VL
    base_oth = dev_of({**pos, "core": 1 - pos["core"]}) * VL

    def zcopy(i):
        return pltpu.make_async_copy(z_in.at[pl.ds(pl.multiple_of(i * TB, TB), TB), :], zb.at[i % 2], zsem.at[i % 2])

    def ocopy(i):
        return pltpu.make_async_copy(dh_s.at[i % 2], dh_out.at[pl.ds(pl.multiple_of(i * TB, TB), TB), :], osem.at[i % 2])

    zcopy(0).start()
    zcopy(1).start()
    dw_own[...] = jnp.zeros_like(dw_own)
    dw_oth[...] = jnp.zeros_like(dw_oth)
    load_w(w_own, w_oth, wt, wsem)
    nsub = CT // 256

    def block(i, carry):
        zcopy(i).wait()

        @pl.when(i >= 2)
        def _():
            ocopy(i - 2).wait()
        zbuf = zb.at[i % 2]
        dhb = dh_s.at[i % 2]
        aux = tok_tile(g2, i, 1).astype(F32)
        lab_s[...] = label_minus_lane(aux)
        wt_s[...] = jnp.broadcast_to(aux[:, 3:4], (TB, 128)) / msum[0:1, :]
        lse_s[...] = jnp.broadcast_to(lse[pl.ds(i, 1), :], (128, TB)).T
        for k, g in enumerate((g0, g1, g2)):
            hT[256 * k:256 * k + 128, :] = tok_tile(g, i, 0).T
            if k < 2:
                hT[256 * k + 128:256 * k + 256, :] = tok_tile(g, i, 1).T

        def make_dz(seg, r):
            half = seg // (NSEG // 2)
            base = (base_own, base_oth)[half] + (seg % (NSEG // 2)) * CT
            rows = pl.ds(r * 16, 16)
            lse_b = lse_s[rows, :]
            w_b = wt_s[rows, :]
            labm = lab_s[rows, :]
            for k in range(CT // 128):
                p = jnp.exp(zbuf[rows, pl.ds(seg * CT + 128 * k, 128)] - lse_b)
                p = jnp.where(labm == base + 128 * k, p - 1.0, p)
                db[seg * (CT // 128) + k, rows, :] = (p * w_b).astype(BF16)

        for r in range(TB // 16):
            make_dz(0, r)
        for seg in range(NSEG):
            piece = 0
            dz = [jnp.concatenate([db[2 * j], db[2 * j + 1]], axis=1) for j in range(seg * nsub, seg * nsub + nsub)]
            ops = []
            for n in range(3):
                ops.append(("h", n))
            for sub in range(nsub):
                ops.append(("w", sub))
            per = -(-(TB // 16) // len(ops))
            for kind, n in ops:
                if kind == "h":
                    lo, hi = 256 * n, min(256 * n + 256, DM)
                    part = None
                    for sub in range(nsub):
                        q = lax.dot_general(dz[sub], w_pair(wt, seg * nsub + sub, lo, hi), (((1,), (1,)), ((), ())), preferred_element_type=F32)
                        part = q if part is None else part + q
                    if seg == 0:
                        dhb[:, lo:hi] = part
                    else:
                        dhb[:, lo:hi] += part
                else:
                    half = seg // (NSEG // 2)
                    off = (seg % (NSEG // 2)) * CT + 256 * n
                    dw_ref = (dw_own, dw_oth)[half]
                    dw_ref[:, off:off + 256] += jnp.dot(hT[...], dz[n], preferred_element_type=F32)
                if seg + 1 < NSEG:
                    for r in range(per):
                        if piece < TB // 16:
                            make_dz(seg + 1, piece)
                            piece += 1
        ocopy(i).start()

        @pl.when(i + 2 < NB)
        def _():
            zcopy(i + 2).start()
        return carry

    lax.fori_loop(0, NB, block, 0)
    ocopy(NB - 2).wait()
    ocopy(NB - 1).wait()


def grads_call(g0, g1, g2, w_own, w_oth, z, lse, msum):
    vm = pl.BlockSpec(memory_space=pltpu.VMEM)
    anyspec = pl.BlockSpec(memory_space=pl.ANY)
    dwshape = jax.ShapeDtypeStruct((DM, VL), F32)
    return pl.pallas_call(
        grads_kernel,
        out_shape=(jax.ShapeDtypeStruct((NTOK, DM), F32), dwshape, dwshape),
        in_specs=[vm] * 3 + [anyspec] * 3 + [vm] * 2,
        out_specs=(anyspec, vm, vm),
        scratch_shapes=[pltpu.VMEM((2, TB, 2 * VL), F32), pltpu.VMEM((2 * VL // 128, TB, 128), BF16), pltpu.VMEM((2 * VL // 128, DM, 128), BF16),
                        pltpu.VMEM((DM, TB), BF16), pltpu.VMEM((2, TB, DM), F32)] + [pltpu.VMEM((TB, 128), F32)] * 2
        + [pltpu.VMEM((TB, 128), jnp.int32), pltpu.SemaphoreType.DMA((2,)), pltpu.SemaphoreType.DMA((2,)), pltpu.SemaphoreType.DMA((2 * VL // 128,))],
        compiler_params=pltpu.CompilerParams(vmem_limit_bytes=VMEM_CAP),
    )(g0, g1, g2, w_own, w_oth, z, lse, msum)


LANES = ((0, 256), (256, 256), (512, 128))


def scatter_kernel(dh, normed, inv_std, gain, lossp, dw_send, dx_out, vec_out, dw_got, *scr):
    bufs = scr[:36]
    vcur, vgot, own_s, ssem, rsem, vssem, vrsem, wsem = scr[36:]
    pos = here()
    barrier_with(ring_peers(pos, (1, 2, 3)))
    wcopy = rcopy(dw_send, dw_got, wsem.at[0], wsem.at[1], shifted(pos, "core", 0))
    wcopy.start()
    half = TOK // 2
    waits = []
    cur = {}

    def view(c, phase, coord, lo):
        lane0, width = LANES[c]
        axis = ORDERS[c][phase]
        rows = pl.ds(lo, half)
        if phase == 0:
            idx = tuple(coord if ax == axis else slice(None) for ax in ("z", "y", "x"))
            return dh.at[idx + (rows, pl.ds(lane0, width))]
        ref, axes = cur[c]
        idx = tuple(coord if ax == axis else slice(None) for ax in axes)
        return ref.at[idx + (rows, slice(None))]

    def add_into(dst, srcs, lead):
        if lead == 0:
            v = dst[...]
            for s in srcs:
                v = v + s[...]
            dst[...] = v
        else:
            def body(j, carry):
                if lead == 1:
                    add_into(dst.at[j], [s.at[j] for s in srcs], 0)
                else:
                    for q in range(SIDE):
                        add_into(dst.at[j, q], [s.at[j, q] for s in srcs], 0)
                return carry
            lax.fori_loop(0, SIDE, body, 0)

    for phase in range(3):
        lead = 2 - phase
        state = []
        for c in range(3):
            axis = ORDERS[c][phase]
            a = pos[axis]
            r1p, r1m, r2p, r2m = bufs[(c * 3 + phase) * 4:(c * 3 + phase) * 4 + 4]
            s0 = (c * 3 + phase) * 6
            pre = (slice(None),) * lead
            right, left = shifted(pos, axis, 1), shifted(pos, axis, -1)
            lo0, lo1 = pre + (pl.ds(0, half), slice(None)), pre + (pl.ds(half, half), slice(None))
            near_r, near_l = (a + 1) % SIDE, (a + SIDE - 1) % SIDE
            far = (a + 2) % SIDE
            sends = [
                rcopy(view(c, phase, far, 0), r1p, ssem.at[s0], rsem.at[s0], right),
                rcopy(view(c, phase, far, half), r1m, ssem.at[s0 + 1], rsem.at[s0 + 1], left),
                rcopy(view(c, phase, near_r, half), r2p.at[lo1], ssem.at[s0 + 2], rsem.at[s0 + 2], right),
                rcopy(view(c, phase, near_l, 0), r2m.at[lo0], ssem.at[s0 + 3], rsem.at[s0 + 3], left),
                rcopy(r1p, r2p.at[lo0], ssem.at[s0 + 4], rsem.at[s0 + 4], right),
                rcopy(r1m, r2m.at[lo1], ssem.at[s0 + 5], rsem.at[s0 + 5], left),
            ]
            for cp in sends[:4]:
                cp.start()
            state.append((sends, r1p, r1m, r2p, r2m, near_r, near_l, a))
        for c in range(3):
            sends, r1p, r1m, r2p, r2m, near_r, near_l, a = state[c]
            sends[0].wait_recv()
            add_into(r1p, [view(c, phase, near_r, 0)], lead)
            sends[4].start()
            sends[1].wait_recv()
            add_into(r1m, [view(c, phase, near_l, half)], lead)
            sends[5].start()
        new = {}
        for c in range(3):
            sends, r1p, r1m, r2p, r2m, near_r, near_l, a = state[c]
            for k in range(2, 6):
                sends[k].wait_recv()
            for lo in (0, half):
                sl = (slice(None),) * lead + (pl.ds(lo, half), slice(None))
                add_into(r2p.at[sl], [r2m.at[sl], view(c, phase, a, lo)], lead)
            axes = tuple(ax for ax in ("z", "y", "x") if ax not in ORDERS[c][:phase + 1])
            new[c] = (r2p, axes)
            waits += sends
        cur.update(new)
    gh = jnp.concatenate([cur[c][0][...] for c in range(3)], axis=1)
    nrm = normed[...]
    dg = jnp.sum(gh * nrm, axis=0, keepdims=True)
    dc = jnp.sum(gh, axis=0, keepdims=True)
    lane_loss = lossp[...]
    for k in range(5):
        own_s[k:k + 1, :] = dg[:, 128 * k:128 * k + 128]
        own_s[5 + k:6 + k, :] = dc[:, 128 * k:128 * k + 128]
    own_s[10:16, :] = jnp.zeros((6, 128), F32)
    own_s[10:11, :] = jnp.sum(lane_loss, axis=0, keepdims=True)
    src = own_s
    slot = 0
    for p, axis in enumerate(("core", "x", "y", "z")):
        deltas = (1,) if axis == "core" else (2, 1, 3)
        cps = []
        for d in deltas:
            cp = rcopy(src, vgot.at[slot], vssem.at[slot], vrsem.at[slot], shifted(pos, axis, d))
            cp.start()
            cps.append((cp, slot))
            slot += 1
        if p == 0:
            q = gh * (1.0 + gain[...])
            cen = q - jnp.mean(q, axis=-1, keepdims=True)
            dx_out[...] = (inv_std[...] * (cen - nrm * jnp.mean(q * nrm, axis=-1, keepdims=True))).astype(BF16)
        for cp, _ in cps:
            cp.wait()
        vals = {d: vgot[s] for d, (_, s) in zip(deltas, cps)}
        if axis == "core":
            tot = src[...] + vals[1]
        else:
            tot = (src[...] + vals[2]) + (vals[1] + vals[3])
        if p < 3:
            vcur[p] = tot
            src = vcur.at[p]
        else:
            vec_out[...] = tot
    for cp in waits:
        cp.wait_send()
    wcopy.wait()


def scatter_call(dh, normed, inv_std, gain, lossp, dw_oth):
    vm = pl.BlockSpec(memory_space=pltpu.VMEM)
    anyspec = pl.BlockSpec(memory_space=pl.ANY)
    half = TOK // 2
    bufs = []
    for c in range(3):
        for phase in range(3):
            lead = (SIDE,) * (2 - phase)
            w = LANES[c][1]
            bufs += [pltpu.VMEM(lead + (half, w), F32)] * 2 + [pltpu.VMEM(lead + (TOK, w), F32)] * 2
    return pl.pallas_call(
        scatter_kernel,
        out_shape=(jax.ShapeDtypeStruct((TOK, DM), BF16), jax.ShapeDtypeStruct((16, 128), F32), jax.ShapeDtypeStruct((DM, VL), F32)),
        in_specs=[vm] * 5 + [anyspec],
        out_specs=(vm, vm, anyspec),
        scratch_shapes=bufs + [pltpu.VMEM((3, 16, 128), F32), pltpu.VMEM((10, 16, 128), F32), pltpu.VMEM((16, 128), F32),
                               pltpu.SemaphoreType.DMA((54,)), pltpu.SemaphoreType.DMA((54,)),
                               pltpu.SemaphoreType.DMA((10,)), pltpu.SemaphoreType.DMA((10,)), pltpu.SemaphoreType.DMA((2,))],
        compiler_params=pltpu.CompilerParams(collective_id=3, has_side_effects=True, vmem_limit_bytes=VMEM_CAP),
    )(dh, normed, inv_std, gain, lossp, dw_oth)


def solution(mesh):
    def per_device(hidden, norm_gain, norm_bias, w_blk, labels, loss_mask):
        x = hidden.reshape(TOK, DM).astype(F32)
        centered = x - jnp.mean(x, axis=-1, keepdims=True)
        inv_std = lax.rsqrt(jnp.mean(centered * centered, axis=-1, keepdims=True) + NORM_EPS)
        normed = centered * inv_std
        h = (normed * (1.0 + norm_gain) + norm_bias).astype(BF16)
        lab = labels.reshape(TOK, 1)
        mask = loss_mask.reshape(TOK, 1)
        lane = lax.broadcasted_iota(jnp.int32, (TOK, 128), 1)
        aux = jnp.where(lane == 0, lab % 256, jnp.where(lane == 1, (lab // 256) % 256, jnp.where(lane == 2, lab // 65536, 0))).astype(F32)
        aux = jnp.where(lane == 3, mask, aux).astype(BF16)
        parts = [jnp.stack([h[:, 0:128], h[:, 128:256]]), jnp.stack([h[:, 256:384], h[:, 384:512]]), jnp.stack([h[:, 512:], aux])]
        g0, g1, g2, w_oth = gather_call(*parts, w_blk)
        g0, g1, g2 = (g.reshape(NTOK // TOK, 2, TOK, 128) for g in (g0, g1, g2))
        z, lse_loc, mt, ms = logits_call(g0, g1, g2, w_blk, w_oth)
        lse, msum = lse_call(lse_loc, ms)
        dh, dw_own, dw_oth = grads_call(g0, g1, g2, w_blk, w_oth, z, lse, msum)
        chip = lax.axis_index("vp") // 2
        own_lse = lax.dynamic_slice(lse.reshape(NTOK), (chip * TOK,), (TOK,))
        loss_lane = jnp.concatenate([mask[:, 0] * own_lse, jnp.zeros((64,), F32)]).reshape(1, 128)
        lossp = jnp.concatenate([-mt, loss_lane, jnp.zeros((7, 128), F32)])
        dx, vec, dw_got = scatter_call(dh.reshape(SIDE, SIDE, SIDE, TOK, DM), normed, jnp.broadcast_to(inv_std, (TOK, DM)),
                                       norm_gain.reshape(1, DM), lossp, dw_oth)
        grad_w = dw_own + dw_got
        loss = jnp.sum(vec[10]) / msum[0, 0]
        return (loss.reshape(1), dx.reshape(hidden.shape), grad_w, vec[0:5].reshape(DM), vec[5:10].reshape(DM))

    tok_spec = P("vp", "dp")
    return jax.shard_map(
        per_device,
        mesh=mesh,
        in_specs=(P("vp", "dp", None), P(None), P(None), P(None, "vp"), tok_spec, tok_spec),
        out_specs=(P("dp"), P("vp", "dp", None), P("dp", "vp"), P("dp"), P("dp")),
        check_vma=False,
    )
```
